128 devices in a mesh: ia: 16 (over y, z), ja: 8 (over x, core).
Axes of the slice: x: 4, y: 4, z: 4, core: 2. Of those that a mesh axis runs over, the one named last changes fastest.
Arguments:
- basis: bfloat16 [32, 16, 1024, 256], P('ia', 'ja'), may hold values from -0.1875 to 0.1875
- amplitudes: float32 [32, 16, 256, 256], P('ia', 'ja'), may hold values from -6 to 6
- integrals: float32 [32, 16, 256, 256], P('ia', 'ja'), may hold values from -6 to 6
- virt_energy: float32 [1024], replicated, may hold values from 0.05 to 2
- fock: float32 [32, 32], replicated, may hold values from -3 to 3
- occ_energy: float32 [16], P('ja'), may hold values from -2 to -0.2
- blocks: int32 [32, 16], P(None, 'ja'), may hold values from 1 to 2
- couplings: int32 [32, 16, 4], P(None, 'ja'), may hold values from 0 to 31, as said below
Outputs:
- new_amplitudes: float32 [32, 16, 256, 256], P('ia', 'ja')
The draws below stay inside these ranges and needn't reach their ends.
Inputs may be any that keep to these rules, and one draw needn't show every extreme that they name: `couplings`: A pair's 4 entries name different k, none equal to the pair's own i, and no two in the same block of 2 consecutive first orbitals held by one index of ia. Of the 16 entries of the pairs that one device holds, exactly 1 name a k in each such block.
All inputs are finite; a program needn't handle non-finite values.
Results may differ from the reference program's by a relative error of at most 0.0031.
Values may be sent and summed in bfloat16 or wider, within the bound.
No kernel may reach another device: no remote copies, remote signals or barrier semaphores. Data moves between devices by JAX's collectives and lax.ppermute only.
A program may use at most 128 MiB of HBM per device.

```python
import math
import jax
import jax.numpy as jnp
from jax import lax

NPROJ = 1024
NPNO = 256
BLOCK = 128
NCOUPLE = 4
OI_DEV = 2
OJ_DEV = 2
SWEEPS = 2
NI = 32
NJ = 16
N_IA = 16
N_JA = 8


def slot_order(slot_key):
    return jax.random.permutation(slot_key, NCOUPLE)


def draw_couplings(key, part):
    per_device = OI_DEV * OJ_DEV
    key_list = jax.random.split(key, N_IA * N_JA)
    row_ids = jnp.repeat(jnp.arange(N_IA, dtype=jnp.int32), N_JA)

    def one_device(device_key, row_group):
        split_keys = jax.random.split(device_key, 5)
        pair_order = jax.random.permutation(split_keys[0], per_device).astype(jnp.int32)
        within = jax.vmap(slot_order)(jax.random.split(split_keys[1], per_device)).astype(jnp.int32)
        position = NCOUPLE * pair_order[:, None] + within
        targets = jax.random.permutation(split_keys[2], N_IA).astype(jnp.int32)
        block_id = targets[position % N_IA]
        pair_row = (jnp.arange(per_device, dtype=jnp.int32) // OJ_DEV)[:, None]
        other_row = (pair_row + 1 + jax.random.randint(split_keys[3], (per_device, NCOUPLE), 0, OI_DEV - 1)) % OI_DEV
        any_row = jax.random.randint(split_keys[4], (per_device, NCOUPLE), 0, OI_DEV)
        offset_row = jnp.where(block_id == row_group, other_row, any_row)
        return (block_id * OI_DEV + offset_row).astype(jnp.int32).reshape(OI_DEV, OJ_DEV, NCOUPLE)
    pieces = jax.vmap(one_device)(key_list, row_ids)
    pieces = pieces.reshape(N_IA, N_JA, OI_DEV, OJ_DEV, NCOUPLE).transpose(0, 2, 1, 3, 4)
    return pieces.reshape(N_IA * OI_DEV, N_JA * OJ_DEV, NCOUPLE)


def touch_ends(array, rng, smallest, high):
    place = [jax.random.randint(jax.random.fold_in(rng, axis), (), 0, length) for axis, length in enumerate(array.shape)]
    longest = array.shape.index(max(array.shape))
    next_to = place[:longest] + [(place[longest] + 1) % array.shape[longest]] + place[longest + 1:]
    return array.at[tuple(place)].set(smallest).at[tuple(next_to)].set(high)


def steps_of(stream_key, dims, cuts, smallest, high):
    level, own = 1.0, jax.random.fold_in(stream_key, 6)
    for dim, parts in cuts:
        heights = jnp.exp(jax.random.uniform(jax.random.fold_in(own, dim), (parts,), jnp.float32, smallest / len(cuts), high / len(cuts)))
        level = level * jnp.repeat(heights, dims[dim] // parts).reshape([-1 if axis == dim else 1 for axis in range(len(dims))])
    return level


def gaussian(rng, shape, deviation, most, cuts=(), kind=jnp.bfloat16):
    values = deviation * jax.random.normal(rng, shape, jnp.float32)
    if cuts:
        values = values * steps_of(rng, shape, cuts, -0.22, 0.18)
    return jnp.clip(values, -most, most).astype(kind)


def setup_inputs(seed: int = 0) -> dict:
    streams_of = jax.random.split(jax.random.key(seed), 9)
    return {
        "basis": gaussian(streams_of[0], (NI, NJ, NPROJ, NPNO), NPROJ ** -0.5, 0.1875, ((0, 16), (1, 8))),
        "amplitudes": gaussian(streams_of[1], (NI, NJ, NPNO, NPNO), 1.0, 6.0, ((0, 16), (1, 8)), jnp.float32),
        "integrals": gaussian(streams_of[2], (NI, NJ, NPNO, NPNO), 1.0, 6.0, ((0, 16), (1, 8)), jnp.float32),
        "virt_energy": jnp.clip(jnp.exp(jax.random.uniform(streams_of[3], (NPROJ,), jnp.float32, math.log(0.05), math.log(2.0))), 0.05, 2.0),
        "fock": gaussian(streams_of[4], (NI, NI), 0.5, 3.0, (), jnp.float32),
        "occ_energy": jnp.clip(-2.0 + 1.8 * jax.random.uniform(streams_of[5], (NJ,), jnp.float32) ** steps_of(streams_of[5], (NJ,), ((0, 8),), -0.2, 0.2), -2.0, -0.2),
        "blocks": touch_ends(jax.random.randint(streams_of[6], (NI, NJ), 1, NPNO // BLOCK + 1), jax.random.fold_in(streams_of[6], 1), 1, (NPNO // BLOCK + 1) - 1).astype(jnp.int32),
        "couplings": draw_couplings(jax.random.fold_in(streams_of[8], 71), 0),
    }


clip_share = 0.4
denominator_floor = 1.0

def rounded_wide(values):
    return lax.optimization_barrier(values.astype(jnp.bfloat16)).astype(jnp.float32)

def reference(basis, amplitudes, integrals, virt_energy, fock, occ_energy, blocks, couplings):
    orbital_index = jnp.arange(NPNO, dtype=jnp.int32)
    column_mask = orbital_index[None, None, :] < (blocks * BLOCK)[:, :, None]
    masked = basis * column_mask[:, :, None, :].astype(jnp.bfloat16)
    pair_mask = (column_mask[:, :, :, None] & column_mask[:, :, None, :]).astype(jnp.float32)
    row_ids = jnp.arange(NI, dtype=jnp.int32)
    weights = fock[row_ids[:, None, None], couplings]
    energy_shift = jnp.diagonal(fock)[:, None] + occ_energy[None, :]
    pair_ids = jnp.arange(NI * NJ, dtype=jnp.int32)

    def prepare(pair_id):
        row_id = pair_id // NJ
        column_id = pair_id % NJ
        own_basis = masked[row_id, column_id].astype(jnp.float32)
        partners = masked[couplings[row_id, column_id], column_id].astype(jnp.float32)
        intersection = jnp.einsum('xa,sxb->sab', own_basis, partners, precision=lax.Precision.HIGHEST).astype(jnp.bfloat16)
        scaled = rounded_wide(own_basis * virt_energy[:, None])
        virtual = jnp.einsum('xa,xb->ab', own_basis, scaled, precision=lax.Precision.HIGHEST)
        return (intersection, virtual)
    intersections, virtuals = lax.map(prepare, pair_ids)
    diagonal_part = jnp.diagonal(virtuals, axis1=1, axis2=2).reshape(NI, NJ, NPNO)
    denominators = jnp.maximum(diagonal_part[:, :, :, None] + diagonal_part[:, :, None, :] - energy_shift[:, :, None, None], denominator_floor)
    current = amplitudes * pair_mask
    for sweep_index in range(SWEEPS):
        rounded = current.astype(jnp.bfloat16)

        def update_of(pair_id):
            row_id = pair_id // NJ
            column_id = pair_id % NJ
            intersection = intersections[pair_id].astype(jnp.float32)
            partner_amplitudes = rounded[couplings[row_id, column_id], column_id].astype(jnp.float32)
            first_product = rounded_wide(jnp.einsum('sab,sbc->sac', intersection, partner_amplitudes, precision=lax.Precision.HIGHEST))
            second_product = jnp.einsum('sac,sdc->sad', first_product, intersection, precision=lax.Precision.HIGHEST)
            coupled = jnp.einsum('sad,s->ad', second_product, weights[row_id, column_id], precision=lax.Precision.HIGHEST)
            amplitude_block = rounded[row_id, column_id].astype(jnp.float32)
            virtual_block = rounded_wide(virtuals[pair_id])
            local_terms = jnp.dot(virtual_block, amplitude_block, precision=lax.Precision.HIGHEST) + jnp.dot(amplitude_block, virtual_block, precision=lax.Precision.HIGHEST)
            residual = integrals[row_id, column_id] + local_terms - energy_shift[row_id, column_id] * current[row_id, column_id] - coupled
            return pair_mask[row_id, column_id] * residual / denominators[row_id, column_id]
        update = lax.map(update_of, pair_ids).reshape(NI, NJ, NPNO, NPNO)
        squares = jnp.sum(update * update)
        factor = jnp.minimum(1.0, clip_share * NPNO / jnp.sqrt(squares / (NI * NJ) + 1e-06))
        current = current - factor * update
    return current
```

```python
import jax
import jax.numpy as jnp
from jax import lax
from jax.experimental import pallas as pl
from jax.experimental.pallas import tpu as pltpu
from jax.sharding import Mesh
from jax.sharding import PartitionSpec as P

BLOCK = 128
NCOUPLE = 4
NPNO = 256
NPROJ = 1024
ROWS = 2
COLS = 2
PAIRS = ROWS * COLS
REQ = PAIRS * NCOUPLE
PACK = NPROJ + NPNO
HALF = PACK // 2
RING = 4
EARLY = (0, 1, 3)
LATE = 2
DOWN = 2.0**-20

clip_share = 0.4
denominator_floor = 1.0

F32 = jnp.float32
BF16 = jnp.bfloat16
SMEM = pltpu.SMEM
VMEM = pltpu.VMEM
HBM = pltpu.HBM


def spec(space):
    return pl.BlockSpec(memory_space=space)


def grant(mib):
    return pltpu.CompilerParams(vmem_limit_bytes=mib * 2**20)


def dot(a, b):
    return lax.dot_general(a, b, (((1,), (0,)), ((), ())), preferred_element_type=F32)


def dot_nt(a, b):
    return lax.dot_general(a, b, (((1,), (1,)), ((), ())), preferred_element_type=F32)


def pair_mask(live):
    row = lax.broadcasted_iota(jnp.int32, (NPNO, NPNO), 0)
    col = lax.broadcasted_iota(jnp.int32, (NPNO, NPNO), 1)
    return (row < live) & (col < live)


def rel_of(block, y, z):
    return (block // RING - y + RING) % RING, (block % RING - z + RING) % RING


def pack_kernel(
    group, couplings, blocks, basis, amplitudes,
    along_a, along_b, across_a, across_b, sources, own, relative, along_table, across_table,
    staged, current_in, basis_sems, amp_sems, out_sems
):
    mine = group[0]
    y, z = mine // RING, mine % RING
    for q in range(PAIRS):
        pltpu.make_async_copy(basis.at[q], staged.at[q, pl.ds(0, NPROJ)], basis_sems.at[q]).start()
    for q in range(PAIRS):
        pltpu.make_async_copy(amplitudes.at[q], current_in.at[q], amp_sems.at[q]).start()
    outs = ((along_a, 0, 0), (along_b, 2, 0), (across_a, 0, HALF), (across_b, 2, HALF))
    copies = [
        pltpu.make_async_copy(staged.at[pl.ds(first, 2), pl.ds(at, HALF)], out, out_sems.at[i])
        for i, (out, first, at) in enumerate(outs)
    ]
    for q in range(PAIRS):
        pltpu.make_async_copy(basis.at[q], staged.at[q, pl.ds(0, NPROJ)], basis_sems.at[q]).wait()
    copies[0].start()
    copies[1].start()
    for q in range(PAIRS):
        pltpu.make_async_copy(amplitudes.at[q], current_in.at[q], amp_sems.at[q]).wait()
        live = blocks[q % COLS, mine * ROWS + q // COLS] * BLOCK
        staged[q, NPROJ:, :] = jnp.where(pair_mask(live), current_in[q], 0.0).astype(BF16)
    copies[2].start()
    copies[3].start()

    for e in range(REQ):
        row, col, slot = e // (COLS * NCOUPLE), e // NCOUPLE % COLS, e % NCOUPLE
        block = couplings[col, slot, mine * ROWS + row] // ROWS
        own[e] = block
        u, t = rel_of(block, y, z)
        relative[e] = u * RING + t

    def tables(s, carry):
        down = (y + s) % RING * RING + z
        over = y * RING + (z + s) % RING
        for e in range(REQ):
            row, col, slot = e // (COLS * NCOUPLE), e // NCOUPLE % COLS, e % NCOUPLE
            k = couplings[col, slot, down * ROWS + row]
            u, t = rel_of(k // ROWS, y, z)
            along_table[jnp.where(u == 0, s * RING + t, REQ)] = (k % ROWS) * COLS + col
            k = couplings[col, slot, over * ROWS + row]
            u, t = rel_of(k // ROWS, y, z)
            across_table[jnp.where(t == 0, s * RING + u, REQ)] = (k % ROWS) * COLS + col
        return carry

    lax.fori_loop(0, RING, tables, 0)

    def find(d, carry):
        source = jnp.int32(0)
        for e in range(REQ):
            row, col, slot = e // (COLS * NCOUPLE), e // NCOUPLE % COLS, e % NCOUPLE
            k = couplings[col, slot, d * ROWS + row]
            source = jnp.where(k // ROWS == mine, (k % ROWS) * COLS + col, source)
        sources[d] = source
        return carry

    lax.fori_loop(0, REQ, find, 0)
    for copy in copies:
        copy.wait()


def select_kernel(*refs, slots):
    count = len(slots)
    tables, refs = refs[:2], refs[2:]
    gathered, refs = refs[: 4 * count], refs[4 * count :]
    sends, refs = refs[:6], refs[6:]
    staged, in_sems, out_sems = refs
    for i in range(2 * count):
        for part in range(2):
            at = 2 * i + part
            pltpu.make_async_copy(gathered[at], staged.at[i, pl.ds(2 * part, 2)], in_sems.at[at]).start()
    for i in range(2 * count):
        half, slot = i // count, slots[i % count]
        for part in range(2):
            at = 2 * i + part
            pltpu.make_async_copy(gathered[at], staged.at[i, pl.ds(2 * part, 2)], in_sems.at[at]).wait()
        for s in range(1, RING):
            q = tables[half][s * RING + slot]
            pltpu.make_async_copy(
                staged.at[i, q], sends[half * 3 + s - 1].at[i % count], out_sems.at[i * 3 + s - 1]
            ).start()
    for i in range(2 * count):
        for s in range(1, RING):
            pltpu.make_async_copy(
                staged.at[i, 0], sends[i // count * 3 + s - 1].at[i % count], out_sems.at[i * 3 + s - 1]
            ).wait()


def local_kernel(group, blocks, fock, occ, energy, basis, amplitudes, integrals, turned, virtual, scale, residual, start):
    eye = lax.broadcasted_iota(jnp.int32, (NPNO, NPNO), 0) == lax.broadcasted_iota(jnp.int32, (NPNO, NPNO), 1)
    for q in range(PAIRS):
        row = group[0] * ROWS + q // COLS
        live = blocks[q % COLS, row] * BLOCK
        shift = fock[row, row] + occ[q % COLS]
        current = jnp.where(pair_mask(live), amplitudes[q], 0.0)
        start[q] = current
        rounded = current.astype(BF16)
        basis_t = basis[q].T
        turned[q] = basis_t
        scaled_t = (basis_t.astype(F32) * energy[...]).astype(BF16)
        wide = dot_nt(basis_t, scaled_t)
        rounded_wide = wide.astype(BF16)
        virtual[q] = rounded_wide
        diagonal = jnp.where(eye, wide, 0.0)
        down = jnp.sum(diagonal, axis=1, keepdims=True)
        along = jnp.sum(diagonal, axis=0, keepdims=True)
        denominators = jnp.maximum(down + along - shift, denominator_floor)
        scale[q] = jnp.where(pair_mask(live), 1.0 / denominators, 0.0)
        residual[q] = integrals[q] + dot(rounded_wide, rounded) + dot(rounded, rounded_wide) - shift * current


def weights_of(group, couplings, fock, p):
    row = group[0] * ROWS + p // COLS
    return [fock[row, couplings[p % COLS, s, row]] for s in range(NCOUPLE)]


def coupled_of(blocks, partners, weights):
    total = None
    for block, partner, weight in zip(blocks, partners, weights):
        second = weight * dot_nt(dot(block, partner).astype(BF16), block)
        total = second if total is None else total + second
    return total


def first_kernel(*refs):
    group, couplings, sources, relative, along_table, across_table, fock, turned, residual, scale = refs[:10]
    gathered, taken, relayed = refs[10:26], refs[26:32], refs[32:38]
    overlap, update, send, staged, kept, in_sems, overlap_sems, out_sems = refs[38:]
    for half, table in enumerate((along_table, across_table)):
        rows = pl.ds(half * HALF, HALF)
        for u in range(RING):
            for t in range(RING):
                r = u * RING + t
                far, near = (u, t) if half == 0 else (t, u)
                target, sem = staged.at[r, rows], in_sems.at[half * REQ + r]
                if far == 0:
                    q = table[near]
                    for part in range(2):

                        @pl.when(q // 2 == part)
                        def _():
                            source = gathered[half * 8 + near * 2 + part]
                            pltpu.make_async_copy(source.at[q % 2], target, sem).start()
                elif near == LATE:
                    pltpu.make_async_copy(relayed[half * 3 + far - 1].at[0], target, sem).start()
                else:
                    source = taken[half * 3 + far - 1]
                    pltpu.make_async_copy(source.at[EARLY.index(near)], target, sem).start()

    def keep(e):
        return pltpu.make_async_copy(kept_overlap.at[e], overlap.at[e], overlap_sems.at[e])

    kept_overlap, kept_update = kept
    for p in range(PAIRS):
        arrived = []
        for s in range(NCOUPLE):
            r = relative[p * NCOUPLE + s]
            for half in range(2):
                part = staged.at[0, pl.ds(half * HALF, HALF)]
                pltpu.make_async_copy(part, part, in_sems.at[half * REQ + r]).wait()
            arrived.append(r)
        blocks = [dot(turned[p], staged[r, :NPROJ, :]).astype(BF16) for r in arrived]
        for s, block in enumerate(blocks):
            kept_overlap[p * NCOUPLE + s] = block
            keep(p * NCOUPLE + s).start()
        coupled = coupled_of(blocks, [staged[r, NPROJ:, :] for r in arrived], weights_of(group, couplings, fock, p))
        fresh = scale[p] * (residual[p] - coupled)
        update[p] = fresh
        kept_update[p] = fresh.astype(BF16)
        for d in range(REQ):

            @pl.when(sources[d] == p)
            def _():
                pltpu.make_async_copy(kept_update.at[p], send.at[d], out_sems.at[d]).start()

    for d in range(REQ):
        pltpu.make_async_copy(kept_update.at[0], send.at[d], out_sems.at[d]).wait()
        keep(d).wait()


def linear_kernel(group, fock, occ, virtual, update, linear):
    for p in range(PAIRS):
        row = group[0] * ROWS + p // COLS
        shift = fock[row, row] + occ[p % COLS]
        rounded = update[p].astype(BF16)
        linear[p] = dot(virtual[p], rounded) + dot(rounded, virtual[p]) - shift * update[p]


def total_of(value):
    lanes = jnp.sum(value, axis=0, keepdims=True)
    return jnp.sum(lanes, axis=1, keepdims=True)


def folded(value):
    return jnp.sum(value.reshape(NPNO // 8, 8, NPNO), axis=0)


def second_kernel(
    group, own, couplings, fock, overlap, a0, a1, a2, a3, linear, scale, update, step, sums, held
):
    p = pl.program_id(0)
    blocks = [overlap[s] for s in range(NCOUPLE)]
    coupled = coupled_of(blocks, [a[0] for a in (a0, a1, a2, a3)], weights_of(group, couplings, fock, p))
    change = scale[0] * (linear[0] - coupled)
    step[p] = change
    small = change * DOWN
    before = update[0]

    @pl.when(p == 0)
    def _():
        held[...] = jnp.zeros_like(held)

    for at, value in enumerate((before * before, before * small, small * small)):
        held[at] += folded(value)

    @pl.when(p == PAIRS - 1)
    def _():
        lane = lax.broadcasted_iota(jnp.int32, (1, 128), 1)
        packed = jnp.zeros((1, 128), F32)
        for at in range(3):
            packed = jnp.where(lane == at, total_of(held[at]), packed)
        sums[...] = jnp.broadcast_to(packed, sums.shape)


def clip_of(squares, pairs):
    return jnp.minimum(1.0, clip_share * NPNO / jnp.sqrt(squares / pairs + 1e-06))


def last_kernel(gathered, start, update, step, out, *, pairs):
    summed = jnp.sum(gathered[...], axis=0, keepdims=True)
    lane = lax.broadcasted_iota(jnp.int32, (1, 128), 1)
    first, cross, second = (
        jnp.sum(jnp.where(lane == at, summed, 0.0), axis=1, keepdims=True) for at in range(3)
    )
    factor = clip_of(first, pairs)
    wide = factor / DOWN
    squares = jnp.maximum(first + wide * (wide * second - 2.0 * cross), 0.0)
    other = clip_of(squares, pairs)
    for p in range(PAIRS):
        fresh = update[p] - factor * step[p]
        out[p] = start[p] - factor * update[p] - other * fresh


def arrival_spec(slot):
    return pl.BlockSpec((1, NPNO, NPNO), lambda p, group, own: (own[p * NCOUPLE + slot], 0, 0))


def square_spec():
    return pl.BlockSpec((1, NPNO, NPNO), lambda p, group, own: (p, 0, 0))


def shifted(value, axis, shift):
    return lax.ppermute(value, axis, [(i, (i + shift) % RING) for i in range(RING)])


def select(tables, gathered, slots, name):
    count = len(slots)
    return pl.pallas_call(
        lambda *refs: select_kernel(*refs, slots=slots),
        out_shape=(jax.ShapeDtypeStruct((count, HALF, NPNO), BF16),) * 6,
        in_specs=[spec(SMEM)] * 2 + [spec(HBM)] * (4 * count),
        out_specs=(spec(HBM),) * 6,
        scratch_shapes=[
            VMEM((2 * count, PAIRS, HALF, NPNO), BF16), pltpu.SemaphoreType.DMA((4 * count,)),
            pltpu.SemaphoreType.DMA((6 * count,)),
        ],
        cost_estimate=pl.CostEstimate(flops=10**6, transcendentals=0, bytes_accessed=count * 5 * 2**20),
        compiler_params=grant(4 + 3 * count),
        name=name,
    )(*tables, *gathered)


def shards(basis, amplitudes, integrals, virt_energy, fock, occ_energy, blocks, couplings):
    axes = ("y", "z", "x", "c")
    devices = lax.axis_size(axes)
    pairs = devices * PAIRS
    group = lax.axis_index(("y", "z")).astype(jnp.int32).reshape(1)
    basis = basis.reshape(PAIRS, NPROJ, NPNO)
    amplitudes = amplitudes.reshape(PAIRS, NPNO, NPNO)
    integrals = integrals.reshape(PAIRS, NPNO, NPNO)
    couplings = couplings.transpose(1, 2, 0)
    blocks = blocks.transpose(1, 0)
    square = VMEM((PAIRS, NPNO, NPNO), F32)
    half = jax.ShapeDtypeStruct((2, HALF, NPNO), BF16)
    index = jax.ShapeDtypeStruct((REQ,), jnp.int32)
    table = jax.ShapeDtypeStruct((2 * REQ,), jnp.int32)
    base = NPROJ * NPNO * NPNO * 2
    small = NPNO * NPNO * NPNO * 2

    *halves, sources, own, relative, along_table, across_table = pl.pallas_call(
        pack_kernel,
        out_shape=(half,) * 4 + (index,) * 3 + (table,) * 2,
        in_specs=[spec(SMEM)] * 3 + [spec(HBM)] * 2,
        out_specs=(spec(HBM),) * 4 + (spec(SMEM),) * 5,
        scratch_shapes=[
            VMEM((PAIRS, PACK, NPNO), BF16), VMEM((PAIRS, NPNO, NPNO), F32),
            pltpu.SemaphoreType.DMA((PAIRS,)), pltpu.SemaphoreType.DMA((PAIRS,)), pltpu.SemaphoreType.DMA((4,)),
        ],
        cost_estimate=pl.CostEstimate(flops=10**6, transcendentals=0, bytes_accessed=6 * 2**20),
        compiler_params=grant(8),
        name="pack",
    )(group, couplings, blocks, basis, amplitudes)
    tables = (along_table, across_table)

    rings = (("z", halves[:2]), ("y", halves[2:]))
    ahead = [(shifted(a, axis, 1), shifted(b, axis, 3)) for axis, (a, b) in rings]
    beside = [(shifted(a, axis, 3), shifted(b, axis, 1)) for axis, (a, b) in rings]
    relayed = [(shifted(a, axis, 1), shifted(b, axis, 3)) for (axis, _), (a, b) in zip(rings, ahead)]
    gathered = []
    for (_, own_parts), (a3, b1), (a1, b3), late in zip(rings, ahead, beside, relayed):
        gathered.append((tuple(own_parts), (a1, b1), tuple(late), (a3, b3)))

    turned, virtual, scale, residual, start = pl.pallas_call(
        local_kernel,
        out_shape=(VMEM((PAIRS, NPNO, NPROJ), BF16), VMEM((PAIRS, NPNO, NPNO), BF16), square, square, square),
        in_specs=[spec(SMEM)] * 4 + [spec(VMEM)] * 4,
        out_specs=(spec(VMEM),) * 5,
        cost_estimate=pl.CostEstimate(
            flops=PAIRS * (base + 2 * small), transcendentals=0, bytes_accessed=9 * 2**20
        ),
        compiler_params=grant(16),
        name="local",
    )(group, blocks, fock, occ_energy, virt_energy.reshape(1, NPROJ), basis, amplitudes, integrals)

    early = select(tables, [part for g in gathered for t in EARLY for part in g[t]], EARLY, "early")
    taken = [shifted(v, "yz"[i // 3], i % 3 + 1) for i, v in enumerate(early)]
    late = select(tables, [part for g in gathered for part in g[LATE]], (LATE,), "late")
    relays = [shifted(v, "yz"[i // 3], i % 3 + 1) for i, v in enumerate(late)]
    taken = [taken[h * 3 + 3 - far] for h in range(2) for far in range(1, RING)]
    relays = [relays[h * 3 + 3 - far] for h in range(2) for far in range(1, RING)]

    overlap, update, send_update = pl.pallas_call(
        lambda *refs: first_kernel(*refs[:42], refs[42:44], *refs[44:]),
        in_specs=[spec(SMEM)] * 7 + [spec(VMEM)] * 3 + [spec(HBM)] * 28,
        out_specs=(spec(HBM), spec(VMEM), spec(HBM)),
        scratch_shapes=[
            VMEM((REQ, PACK, NPNO), BF16), VMEM((REQ, NPNO, NPNO), BF16), VMEM((PAIRS, NPNO, NPNO), BF16),
            pltpu.SemaphoreType.DMA((2 * REQ,)), pltpu.SemaphoreType.DMA((REQ,)), pltpu.SemaphoreType.DMA((REQ,)),
        ],
        out_shape=(
            jax.ShapeDtypeStruct((REQ, NPNO, NPNO), BF16), square, jax.ShapeDtypeStruct((REQ, NPNO, NPNO), BF16),
        ),
        cost_estimate=pl.CostEstimate(
            flops=REQ * (base + 2 * small), transcendentals=0, bytes_accessed=20 * 2**20
        ),
        compiler_params=grant(24),
        name="first",
    )(
        group, couplings, sources, relative, *tables, fock, turned, residual, scale,
        *[part for g in gathered for t in g for part in t], *taken, *relays,
    )
    arrived_update = lax.all_to_all(send_update, ("y", "z"), split_axis=0, concat_axis=0, tiled=True)

    linear = pl.pallas_call(
        linear_kernel,
        out_shape=jax.ShapeDtypeStruct((PAIRS, NPNO, NPNO), F32),
        in_specs=[spec(SMEM)] * 3 + [spec(VMEM)] * 2,
        out_specs=spec(VMEM),
        cost_estimate=pl.CostEstimate(flops=PAIRS * 2 * small, transcendentals=0, bytes_accessed=3 * 2**20),
        compiler_params=grant(12),
        name="linear",
    )(group, fock, occ_energy, virtual, update)

    step, sums = pl.pallas_call(
        second_kernel,
        grid_spec=pltpu.PrefetchScalarGridSpec(
            num_scalar_prefetch=2,
            grid=(PAIRS,),
            in_specs=[spec(SMEM)] * 2
            + [pl.BlockSpec((NCOUPLE, NPNO, NPNO), lambda p, group, own: (p, 0, 0))]
            + [arrival_spec(s) for s in range(NCOUPLE)] + [square_spec()] * 3,
            out_specs=(spec(VMEM), spec(VMEM)),
            scratch_shapes=[VMEM((3, 8, NPNO), F32)],
        ),
        out_shape=(square, jax.ShapeDtypeStruct((devices, 128), F32)),
        cost_estimate=pl.CostEstimate(flops=REQ * 2 * small, transcendentals=0, bytes_accessed=9 * 2**20),
        compiler_params=grant(20),
        name="second",
    )(group, own, couplings, fock, overlap, *[arrived_update] * 4, linear, scale, update)
    gathered_sums = lax.all_to_all(sums, axes, split_axis=0, concat_axis=0, tiled=True)

    out = pl.pallas_call(
        lambda *refs: last_kernel(*refs, pairs=pairs),
        out_shape=jax.ShapeDtypeStruct((PAIRS, NPNO, NPNO), F32),
        in_specs=[spec(VMEM)] * 4,
        out_specs=spec(VMEM),
        compiler_params=grant(12),
        name="last",
    )(gathered_sums, start, update, step)
    return out.reshape(ROWS, COLS, NPNO, NPNO)


def solution(mesh):
    finer = Mesh(mesh.devices.reshape(RING, RING, -1, 2), ("y", "z", "x", "c"))
    ia, ja = ("y", "z"), ("x", "c")
    return jax.shard_map(
        shards,
        mesh=finer,
        in_specs=(
            P(ia, ja, None, None),
            P(ia, ja, None, None),
            P(ia, ja, None, None),
            P(),
            P(),
            P(ja),
            P(None, ja),
            P(None, ja, None),
        ),
        out_specs=P(ia, ja, None, None),
        check_vma=False,
    )
```

```python
import jax
import jax.numpy as jnp
from jax import lax
from jax.experimental import pallas as pl
from jax.experimental.pallas import tpu as pltpu
from jax.sharding import Mesh
from jax.sharding import PartitionSpec as P

BLOCK = 128
NCOUPLE = 4
NPNO = 256
NPROJ = 1024
ROWS = 2
COLS = 2
PAIRS = ROWS * COLS
REQ = PAIRS * NCOUPLE
PACK = NPROJ + NPNO
HALF = PACK // 2
REST = NPROJ - HALF
ALL_VMEM = 67043328
FIRST_GRANT = 41
MIDDLE_GRANT = 46
RING = 4
EARLY = (0, 1, 3)
LATE = 2
DOWN = 2.0**-20

clip_share = 0.4
denominator_floor = 1.0

F32 = jnp.float32
BF16 = jnp.bfloat16
SMEM = pltpu.SMEM
VMEM = pltpu.VMEM
HBM = pltpu.HBM


def spec(space):
    return pl.BlockSpec(memory_space=space)


def grant(mib):
    return pltpu.CompilerParams(vmem_limit_bytes=mib * 2**20)


def dot(a, b):
    return lax.dot_general(a, b, (((1,), (0,)), ((), ())), preferred_element_type=F32)


def dot_nt(a, b):
    return lax.dot_general(a, b, (((1,), (1,)), ((), ())), preferred_element_type=F32)


def pair_mask(live):
    row = lax.broadcasted_iota(jnp.int32, (NPNO, NPNO), 0)
    col = lax.broadcasted_iota(jnp.int32, (NPNO, NPNO), 1)
    return (row < live) & (col < live)


def rel_of(block, y, z):
    return ((block >> 2) - y + RING) & 3, ((block & 3) - z + RING) & 3


def pack_kernel(
    group, blocks, basis, amplitudes, along_a, along_b, across_a, across_b,
    staged, current_in, basis_sems, amp_sems, out_sems
):
    for q in range(PAIRS):
        pltpu.make_async_copy(basis.at[q], staged.at[q, pl.ds(0, NPROJ)], basis_sems.at[q]).start()
        pltpu.make_async_copy(amplitudes.at[q], current_in.at[q], amp_sems.at[q]).start()
    outs = (along_a, along_b, across_a, across_b)
    copies = [
        pltpu.make_async_copy(
            staged.at[q, pl.ds(half * HALF, HALF)], outs[half * 2 + q // 2].at[q % 2], out_sems.at[half * PAIRS + q]
        )
        for half in range(2)
        for q in range(PAIRS)
    ]
    for q in range(PAIRS):
        pltpu.make_async_copy(basis.at[q], staged.at[q, pl.ds(0, NPROJ)], basis_sems.at[q]).wait()
        copies[q].start()
        pltpu.make_async_copy(amplitudes.at[q], current_in.at[q], amp_sems.at[q]).wait()
        live = blocks[q % COLS, group[0] * ROWS + q // COLS] * BLOCK
        staged[q, NPROJ:, :] = jnp.where(pair_mask(live), current_in[q], 0.0).astype(BF16)
        copies[PAIRS + q].start()
    for copy in copies:
        copy.wait()


def tables_kernel(
    group, couplings, fock, occ, sources, own, relative, pair_of, along_table, across_table, weights, shifts
):
    mine = group[0]
    y, z = mine >> 2, mine & 3
    for p in range(PAIRS):
        row = mine * ROWS + p // COLS
        shifts[p] = fock[row, row] + occ[p % COLS]
    for e in range(REQ):
        row, col, slot = e // (COLS * NCOUPLE), e // NCOUPLE % COLS, e % NCOUPLE
        k = couplings[col, slot, mine * ROWS + row]
        weights[e] = fock[mine * ROWS + row, k]
        block = k >> 1
        own[e] = block
        u, t = rel_of(block, y, z)
        relative[e] = u * RING + t
        pair_of[u * RING + t] = e // NCOUPLE

    def tables(s, carry):
        down = ((y + s) & 3) * RING + z
        over = y * RING + ((z + s) & 3)
        for e in range(REQ):
            row, col, slot = e // (COLS * NCOUPLE), e // NCOUPLE % COLS, e % NCOUPLE
            k = couplings[col, slot, down * ROWS + row]
            u, t = rel_of(k >> 1, y, z)
            along_table[jnp.where(u == 0, s * RING + t, REQ)] = (k & 1) * COLS + col
            k = couplings[col, slot, over * ROWS + row]
            u, t = rel_of(k >> 1, y, z)
            across_table[jnp.where(t == 0, s * RING + u, REQ)] = (k & 1) * COLS + col
        return carry

    lax.fori_loop(0, RING, tables, 0)

    def find(d, carry):
        source = jnp.int32(0)
        for e in range(REQ):
            row, col, slot = e // (COLS * NCOUPLE), e // NCOUPLE % COLS, e % NCOUPLE
            k = couplings[col, slot, d * ROWS + row]
            source = jnp.where((k >> 1) == mine, (k & 1) * COLS + col, source)
        sources[d] = source
        return carry

    lax.fori_loop(0, REQ, find, 0)


def select_kernel(*refs, slots):
    count = len(slots)
    tables, refs = refs[:2], refs[2:]
    gathered, refs = refs[: 4 * count], refs[4 * count :]
    sends, refs = refs[:6], refs[6:]
    staged, in_sems, out_sems = refs
    for i in range(2 * count):
        for part in range(2):
            at = 2 * i + part
            pltpu.make_async_copy(gathered[at], staged.at[i, pl.ds(2 * part, 2)], in_sems.at[at]).start()
    for i in range(2 * count):
        half, slot = i // count, slots[i % count]
        for part in range(2):
            at = 2 * i + part
            pltpu.make_async_copy(gathered[at], staged.at[i, pl.ds(2 * part, 2)], in_sems.at[at]).wait()
        for s in range(1, RING):
            q = tables[half][s * RING + slot]
            pltpu.make_async_copy(
                staged.at[i, q], sends[half * 3 + s - 1].at[i % count], out_sems.at[i * 3 + s - 1]
            ).start()
    for i in range(2 * count):
        for s in range(1, RING):
            pltpu.make_async_copy(
                staged.at[i, 0], sends[i // count * 3 + s - 1].at[i % count], out_sems.at[i * 3 + s - 1]
            ).wait()


def local_kernel(
    group, blocks, fock, occ, energy, basis, amplitudes, integrals, turned, virtual, scale, residual, start, later
):
    eye = lax.broadcasted_iota(jnp.int32, (NPNO, NPNO), 0) == lax.broadcasted_iota(jnp.int32, (NPNO, NPNO), 1)
    for q in range(PAIRS):
        row = group[0] * ROWS + q // COLS
        live = blocks[q % COLS, row] * BLOCK
        shift = fock[row, row] + occ[q % COLS]
        current = jnp.where(pair_mask(live), amplitudes[q], 0.0)
        start[q] = current
        rounded = current.astype(BF16)
        basis_t = basis[q].T
        turned[q] = basis_t
        scaled_t = (basis_t.astype(F32) * energy[...]).astype(BF16)
        wide = dot_nt(basis_t, scaled_t)
        rounded_wide = wide.astype(BF16)
        virtual[q] = rounded_wide
        diagonal = jnp.where(eye, wide, 0.0)
        down = jnp.sum(diagonal, axis=1, keepdims=True)
        along = jnp.sum(diagonal, axis=0, keepdims=True)
        denominators = jnp.maximum(down + along - shift, denominator_floor)
        scale[q] = jnp.where(pair_mask(live), 1.0 / denominators, 0.0)
        later[q] = scale[q]
        residual[q] = integrals[q] + dot(rounded_wide, rounded) + dot(rounded, rounded_wide) - shift * current


def weights_of(weights, p):
    return [weights[p * NCOUPLE + s] for s in range(NCOUPLE)]


def coupled_of(blocks, partners, weights):
    total = None
    for block, partner, weight in zip(blocks, partners, weights):
        second = weight * dot_nt(dot(block, partner).astype(BF16), block)
        total = second if total is None else total + second
    return total


class Part:
    def __init__(self, half, far, near, sources, at):
        self.half, self.sources, self.at = half, sources, at
        self.rel = far * RING + near if half == 0 else near * RING + far

    def copies(self, source, staged, amps, sems, i):
        if self.half == 0:
            return [pltpu.make_async_copy(source, staged.at[i], sems.at[i, 0])]
        return [
            pltpu.make_async_copy(source.at[pl.ds(0, REST)], staged.at[i, pl.ds(0, REST)], sems.at[i, 0]),
            pltpu.make_async_copy(source.at[pl.ds(REST, NPNO)], amps.at[self.rel], sems.at[i, 1]),
        ]

    def start(self, staged, amps, sems, i):
        if len(self.sources) == 1:
            for copy in self.copies(self.sources[0].at[self.at], staged, amps, sems, i):
                copy.start()
            return
        for which, source in enumerate(self.sources):

            @pl.when(self.at // 2 == which)
            def _():
                for copy in self.copies(source.at[self.at % 2], staged, amps, sems, i):
                    copy.start()

    def wait(self, staged, amps, sems, i):
        for copy in self.copies(self.sources[0].at[0], staged, amps, sems, i):
            copy.wait()

    def product(self, turned, pair, staged, i):
        if self.half == 0:
            return dot(turned[pair, :, :HALF], staged[i])
        return dot(turned[pair, :, HALF:], staged[i, :REST, :])


def products(parts, pair_of, turned, staged, amps, sems):
    for i, part in enumerate(parts):
        part.start(staged, amps, sems, i)
    for i, part in enumerate(parts):
        part.wait(staged, amps, sems, i)
        yield part.rel, part.product(turned, pair_of[part.rel], staged, i)


def near_kernel(*refs):
    pair_of, along_table, across_table, turned = refs[:4]
    gathered = refs[4:20]
    partial, amps, _, staged, sems = refs[20:]
    parts = []
    for near in range(RING):
        for half, table in enumerate((along_table, across_table)):
            at = half * 8 + near * 2
            parts.append(Part(half, 0, near, gathered[at : at + 2], table[near]))
    seen = set()
    for r, product in products(parts, pair_of, turned, staged, amps, sems):
        partial[r] = partial[r] + product if r in seen else product
        seen.add(r)


NEAR = {u * RING for u in range(RING)} | set(range(RING))
OPEN = (6, 9, 11, 14, 10)


def rels_of(fars):
    return {far * RING + near for far in fars for near in EARLY} | {near * RING + far for far in fars for near in EARLY}


def middle_kernel(*refs, fars, before):
    count = 2 * len(fars)
    pair_of, turned = refs[:2]
    taken = refs[6 if before else 4 :][:count]
    partial, amps, ready, rest, _, staged, sems = refs[-7:]
    parts = [
        Part(half, far, near, (taken[half * len(fars) + i],), EARLY.index(near))
        for i, far in enumerate(fars)
        for near in EARLY
        for half in range(2)
    ]
    seen = NEAR | rels_of(before)
    if not before:
        ready[0] = partial[0].astype(BF16)
    for r, product in products(parts, pair_of, turned, staged, amps, sems):
        if r in OPEN:
            rest[OPEN.index(r)] = product
        elif r in seen:
            ready[r] = (partial[r] + product).astype(BF16)
        else:
            partial[r] = product
        seen.add(r)


def first_kernel(*refs):
    sources, relative, pair_of, weights = refs[:4]
    turned, residual, scale, rest, _, _ = refs[4:10]
    relayed = refs[10:16]
    overlap, update, send, amps, ready = refs[16:21]
    staged, kept, fresh_kept, in_sems, overlap_sems, out_sems, update_sems = refs[25:]

    def keep(r):
        return pltpu.make_async_copy(ready.at[r], overlap.at[r], overlap_sems.at[r])

    for r in range(REQ):
        if r not in OPEN:
            keep(r).start()
    parts = [
        Part(half, far, LATE, (relayed[half * 3 + far - 1],), 0) for far in range(1, RING) for half in range(2)
    ]
    held = {}
    for r, product in products(parts, pair_of, turned, staged, amps, in_sems):
        if r == LATE * RING + LATE and r not in held:
            held[r] = product
            continue
        before = held[r] if r in held else rest[OPEN.index(r)]
        ready[r] = (before + product).astype(BF16)
        keep(r).start()
    for p in range(PAIRS):
        arrived = [relative[p * NCOUPLE + s] for s in range(NCOUPLE)]
        blocks = [ready[r] for r in arrived]
        coupled = coupled_of(blocks, [amps[r] for r in arrived], weights_of(weights, p))
        fresh = scale[p] * (residual[p] - coupled)
        fresh_kept[p] = fresh
        pltpu.make_async_copy(fresh_kept.at[p], update.at[p], update_sems.at[p]).start()
        kept[p] = fresh.astype(BF16)
        for d in range(REQ):

            @pl.when(sources[d] == p)
            def _():
                pltpu.make_async_copy(kept.at[p], send.at[d], out_sems.at[d]).start()

    for d in range(REQ):
        pltpu.make_async_copy(kept.at[0], send.at[d], out_sems.at[d]).wait()
        keep(d).wait()
    for p in range(PAIRS):
        pltpu.make_async_copy(fresh_kept.at[p], update.at[p], update_sems.at[p]).wait()


def total_of(value):
    lanes = jnp.sum(value, axis=0, keepdims=True)
    return jnp.sum(lanes, axis=1, keepdims=True)


def folded(value):
    return jnp.sum(value.reshape(NPNO // 8, 8, NPNO), axis=0)


def second_kernel(
    own, relative, weights, shifts, overlap_from, arrived_from, virtual_from, scale_from, update_from, start_from,
    step, sums, update, start, overlap, arrived, virtual, scale, held, sems
):
    copies = []
    for p in range(PAIRS):
        pieces = []
        for e in range(p * NCOUPLE, (p + 1) * NCOUPLE):
            pieces += [(overlap_from.at[relative[e]], overlap.at[e]), (arrived_from.at[own[e]], arrived.at[e])]
        for source, target in (
            (virtual_from, virtual), (scale_from, scale), (update_from, update), (start_from, start)
        ):
            pieces.append((source.at[p], target.at[p]))
        copies.append([pltpu.make_async_copy(*piece, sems.at[p, i]) for i, piece in enumerate(pieces)])
        for copy in copies[p]:
            copy.start()
    for p in range(PAIRS):
        for copy in copies[p]:
            copy.wait()
        entries = range(p * NCOUPLE, (p + 1) * NCOUPLE)
        blocks = [overlap[e] for e in entries]
        coupled = coupled_of(blocks, [arrived[e] for e in entries], weights_of(weights, p))
        before = update[p]
        rounded = before.astype(BF16)
        linear = dot(virtual[p], rounded) + dot(rounded, virtual[p]) - shifts[p] * before
        change = scale[p] * (linear - coupled)
        step[p] = change
        small = change * DOWN
        for at, value in enumerate((before * before, before * small, small * small)):
            held[at] = folded(value) if p == 0 else held[at] + folded(value)
    lane = lax.broadcasted_iota(jnp.int32, (1, 128), 1)
    packed = jnp.zeros((1, 128), F32)
    for at in range(3):
        packed = jnp.where(lane == at, total_of(held[at]), packed)
    sums[...] = jnp.broadcast_to(packed, sums.shape)


def clip_of(squares, pairs):
    return jnp.minimum(1.0, clip_share * NPNO / jnp.sqrt(squares / pairs + 1e-06))


def last_kernel(gathered, start, update, step, out, *_, pairs):
    summed = jnp.sum(gathered[...], axis=0, keepdims=True)
    lane = lax.broadcasted_iota(jnp.int32, (1, 128), 1)
    first, cross, second = (
        jnp.sum(jnp.where(lane == at, summed, 0.0), axis=1, keepdims=True) for at in range(3)
    )
    factor = clip_of(first, pairs)
    wide = factor / DOWN
    squares = jnp.maximum(first + wide * (wide * second - 2.0 * cross), 0.0)
    other = clip_of(squares, pairs)
    for p in range(PAIRS):
        fresh = update[p] - factor * step[p]
        out[p] = start[p] - factor * update[p] - other * fresh


def shifted(value, axis, shift):
    return lax.ppermute(value, axis, [(i, (i + shift) % RING) for i in range(RING)])


def sent(values):
    out = []
    for i, value in enumerate(values):
        axis, shift = "yz"[i // 3], i % 3 + 1
        out.append(shifted(value, axis, shift))
    return out


def select(tables, gathered, slots):
    count = len(slots)
    return pl.pallas_call(
        lambda *refs: select_kernel(*refs, slots=slots),
        out_shape=(jax.ShapeDtypeStruct((count, HALF, NPNO), BF16),) * 6,
        in_specs=[spec(SMEM)] * 2 + [spec(HBM)] * (4 * count),
        out_specs=(spec(HBM),) * 6,
        scratch_shapes=[
            VMEM((2 * count, PAIRS, HALF, NPNO), BF16), pltpu.SemaphoreType.DMA((4 * count,)),
            pltpu.SemaphoreType.DMA((6 * count,)),
        ],
        cost_estimate=pl.CostEstimate(flops=10**6, transcendentals=0, bytes_accessed=count * 5 * 2**20),
        compiler_params=grant(57 if count > 1 else 48),
    )(*tables, *gathered)


def shards(basis, amplitudes, integrals, virt_energy, fock, occ_energy, blocks, couplings):
    axes = ("y", "z", "x", "c")
    devices = lax.axis_size(axes)
    pairs = devices * PAIRS
    group = lax.axis_index(("y", "z")).astype(jnp.int32).reshape(1)
    basis = basis.reshape(PAIRS, NPROJ, NPNO)
    amplitudes = amplitudes.reshape(PAIRS, NPNO, NPNO)
    integrals = integrals.reshape(PAIRS, NPNO, NPNO)
    couplings = couplings.transpose(1, 2, 0)
    blocks = blocks.transpose(1, 0)
    square = VMEM((PAIRS, NPNO, NPNO), F32)
    plain = jax.ShapeDtypeStruct((PAIRS, NPNO, NPNO), F32)
    half = jax.ShapeDtypeStruct((2, HALF, NPNO), BF16)
    index = jax.ShapeDtypeStruct((REQ,), jnp.int32)
    table = jax.ShapeDtypeStruct((2 * REQ,), jnp.int32)
    base = NPROJ * NPNO * NPNO * 2
    small = NPNO * NPNO * NPNO * 2

    halves = pl.pallas_call(
        pack_kernel,
        out_shape=(half,) * 4,
        in_specs=[spec(SMEM)] * 2 + [spec(HBM)] * 2,
        out_specs=(spec(HBM),) * 4,
        scratch_shapes=[
            VMEM((PAIRS, PACK, NPNO), BF16), VMEM((PAIRS, NPNO, NPNO), F32),
            pltpu.SemaphoreType.DMA((PAIRS,)), pltpu.SemaphoreType.DMA((PAIRS,)), pltpu.SemaphoreType.DMA((2 * PAIRS,)),
        ],
        cost_estimate=pl.CostEstimate(flops=10**6, transcendentals=0, bytes_accessed=6 * 2**20),
        compiler_params=pltpu.CompilerParams(vmem_limit_bytes=ALL_VMEM),
        name="pack",
    )(group, blocks, basis, amplitudes)
    sources, own, relative, pair_of, *tables, weights, shifts = pl.pallas_call(
        tables_kernel,
        out_shape=(index,) * 4 + (table,) * 2 + (jax.ShapeDtypeStruct((REQ,), F32), jax.ShapeDtypeStruct((PAIRS,), F32)),
        in_specs=[spec(SMEM)] * 4,
        out_specs=(spec(SMEM),) * 8,
        cost_estimate=pl.CostEstimate(flops=10**7, transcendentals=0, bytes_accessed=2**14),
        compiler_params=pltpu.CompilerParams(vmem_limit_bytes=ALL_VMEM),
        name="tables",
    )(group, couplings, fock, occ_energy)

    rings = (("z", halves[:2]), ("y", halves[2:]))
    ahead = [(shifted(a, axis, 1), shifted(b, axis, 3)) for axis, (a, b) in rings]
    beside = []
    for axis, (a, b) in rings:
        beside.append((shifted(a, axis, 3), shifted(b, axis, 1)))
    relayed = []
    for (axis, _), (a, b) in zip(rings, ahead):
        a = shifted(a, axis, 1)
        b = shifted(b, axis, 3)
        relayed.append((a, b))
    gathered = []
    for (_, own_parts), (a3, b1), (a1, b3), late in zip(rings, ahead, beside, relayed):
        gathered.append((tuple(own_parts), (a1, b1), tuple(late), (a3, b3)))

    turned, virtual, scale, residual, start, scale_later = pl.pallas_call(
        local_kernel,
        out_shape=(
            VMEM((PAIRS, NPNO, NPROJ), BF16), jax.ShapeDtypeStruct((PAIRS, NPNO, NPNO), BF16), square, square, plain, plain,
        ),
        in_specs=[spec(SMEM)] * 4 + [spec(VMEM)] * 4,
        out_specs=(spec(VMEM),) * 6,
        cost_estimate=pl.CostEstimate(flops=PAIRS * (base + 2 * small), transcendentals=0, bytes_accessed=9 * 2**20),
        compiler_params=grant(58),
        name="local",
    )(group, blocks, fock, occ_energy, virt_energy.reshape(1, NPROJ), basis, amplitudes, integrals)

    early = select(tables, [part for g in gathered for t in EARLY for part in g[t]], EARLY)
    taken = sent(early)
    late = select(tables, [part for g in gathered for part in g[LATE]], (LATE,))
    relays = sent(late)
    taken = [taken[h * 3 + 3 - far] for h in range(2) for far in range(1, RING)]
    relays = [relays[h * 3 + 3 - far] for h in range(2) for far in range(1, RING)]

    shares = VMEM((REQ, NPNO, NPNO), F32)
    listed = VMEM((REQ, NPNO, NPNO), BF16)
    turned_shape = VMEM((PAIRS, NPNO, NPROJ), BF16)
    partial, amps, turned = pl.pallas_call(
        near_kernel,
        out_shape=(shares, listed, turned_shape),
        in_specs=[spec(SMEM)] * 3 + [spec(VMEM)] + [spec(HBM)] * 16,
        out_specs=(spec(VMEM),) * 3,
        input_output_aliases={3: 2},
        scratch_shapes=[VMEM((8, HALF, NPNO), BF16), pltpu.SemaphoreType.DMA((8, 2))],
        cost_estimate=pl.CostEstimate(flops=4 * base, transcendentals=0, bytes_accessed=4 * 2**20),
        compiler_params=grant(50),
        name="near",
    )(pair_of, *tables, turned, *[part for g in gathered for t in g for part in t])
    state = (partial, amps)
    for fars, before in (((1, 3), ()), ((2,), (1, 3))):
        inputs = [taken[h * 3 + far - 1] for h in range(2) for far in fars]
        *state, turned = pl.pallas_call(
            lambda *refs, fars=fars, before=before: middle_kernel(*refs, fars=fars, before=before),
            out_shape=(shares, listed, listed, square, turned_shape),
            in_specs=[spec(SMEM)] + [spec(VMEM)] * (1 + len(state)) + [spec(HBM)] * len(inputs),
            out_specs=(spec(VMEM),) * 5,
            scratch_shapes=[
                VMEM((6 * len(fars), HALF, NPNO), BF16), pltpu.SemaphoreType.DMA((6 * len(fars), 2)),
            ],
            input_output_aliases={1: 4} | {2 + k: k for k in range(len(state))},
            cost_estimate=pl.CostEstimate(
                flops=3 * len(fars) * base, transcendentals=0, bytes_accessed=len(fars) * 3 * 2**20
            ),
            compiler_params=grant(MIDDLE_GRANT),
        )(pair_of, turned, *state, *inputs)
    _, amps, ready, rest = state
    overlap, update, send_update, *_ = pl.pallas_call(
        first_kernel,
        in_specs=[spec(SMEM)] * 4 + [spec(VMEM)] * 6 + [spec(HBM)] * 6,
        out_specs=(spec(HBM),) * 3 + (spec(VMEM),) * 6,
        scratch_shapes=[
            VMEM((6, HALF, NPNO), BF16), VMEM((PAIRS, NPNO, NPNO), BF16),
            VMEM((PAIRS, NPNO, NPNO), F32), pltpu.SemaphoreType.DMA((6, 2)), pltpu.SemaphoreType.DMA((REQ,)),
            pltpu.SemaphoreType.DMA((REQ,)), pltpu.SemaphoreType.DMA((PAIRS,)),
        ],
        out_shape=(
            jax.ShapeDtypeStruct((REQ, NPNO, NPNO), BF16), plain, jax.ShapeDtypeStruct((REQ, NPNO, NPNO), BF16),
            listed, listed, turned_shape, square, square, square,
        ),
        input_output_aliases={8: 3, 9: 4, 4: 5, 5: 6, 6: 7, 7: 8},
        cost_estimate=pl.CostEstimate(
            flops=3 * base + REQ * 2 * small, transcendentals=0, bytes_accessed=8 * 2**20
        ),
        compiler_params=grant(FIRST_GRANT),
        name="first",
    )(sources, relative, pair_of, weights, turned, residual, scale, rest, amps, ready, *relays)
    arrived_update = lax.all_to_all(send_update, ("y", "z"), split_axis=0, concat_axis=0, tiled=True)

    step, sums, update, start = pl.pallas_call(
        second_kernel,
        out_shape=(square, jax.ShapeDtypeStruct((devices, 128), F32), square, square),
        in_specs=[spec(SMEM)] * 4 + [spec(HBM)] * 6,
        out_specs=(spec(VMEM),) * 4,
        scratch_shapes=[
            VMEM((REQ, NPNO, NPNO), BF16), VMEM((REQ, NPNO, NPNO), BF16), VMEM((PAIRS, NPNO, NPNO), BF16),
            VMEM((PAIRS, NPNO, NPNO), F32), VMEM((3, 8, NPNO), F32), pltpu.SemaphoreType.DMA((PAIRS, 12)),
        ],
        cost_estimate=pl.CostEstimate(flops=REQ * 2 * small, transcendentals=0, bytes_accessed=9 * 2**20),
        compiler_params=grant(57),
        name="second",
    )(own, relative, weights, shifts, overlap, arrived_update, virtual, scale_later, update, start)
    gathered_sums = lax.all_to_all(sums, axes, split_axis=0, concat_axis=0, tiled=True)

    out, *_ = pl.pallas_call(
        lambda *refs: last_kernel(*refs, pairs=pairs),
        out_shape=(jax.ShapeDtypeStruct((PAIRS, NPNO, NPNO), F32), square, square, square),
        in_specs=[spec(VMEM)] * 4,
        out_specs=(spec(VMEM),) * 4,
        input_output_aliases={1: 1, 2: 2, 3: 3},
        compiler_params=grant(12),
        name="last",
    )(gathered_sums, start, update, step)
    return out.reshape(ROWS, COLS, NPNO, NPNO)


def solution(mesh):
    finer = Mesh(mesh.devices.reshape(RING, RING, -1, 2), ("y", "z", "x", "c"))
    ia, ja = ("y", "z"), ("x", "c")
    return jax.shard_map(
        shards,
        mesh=finer,
        in_specs=(
            P(ia, ja, None, None),
            P(ia, ja, None, None),
            P(ia, ja, None, None),
            P(),
            P(),
            P(ja),
            P(None, ja),
            P(None, ja, None),
        ),
        out_specs=P(ia, ja, None, None),
        check_vma=False,
    )
```
